32 devices in a mesh: row: 4 (over y, x), col: 4 (over z), band: 2 (over core).
Axes of the slice: x: 2, y: 2, z: 4, core: 2. Of those that a mesh axis runs over, the one named last changes fastest.
Arguments:
- freq_index: int32 [2], replicated, may hold values from 0 to 32
- band_energy: float32 [8], replicated, may hold values from -4 to 4
- pole_amp: float32 [4096, 4096], P('row', 'col'), may hold values from -6 to 6
- pole_freq: float32 [4096, 4096], P('row', 'col'), may hold values from 0.5 to 4
- left_pieces: bfloat16 [8, 256, 4096], P(('col', 'band'), None, 'row'), may hold values from -0.055664062 to 0.055664062
- right_pieces: bfloat16 [8, 256, 4096], P(('row', 'band'), None, 'col'), may hold values from -0.055664062 to 0.055664062
Outputs:
- sigma: float32 [2, 256, 256], P(None, ('row', 'col', 'band'))
The draws below stay inside these ranges and needn't reach their ends.
All inputs are finite; a program needn't handle non-finite values.
Results may differ from the reference program's by a relative error of at most 0.0055.
Values may be sent and summed in bfloat16 or wider, within the bound.
No kernel may reach another device: no remote copies, remote signals or barrier semaphores. Data moves between devices by JAX's collectives and lax.ppermute only.
A program may use at most 128 MiB of HBM per device.

```python
import math
import jax
import jax.numpy as jnp
from jax import lax

TILE = 1024
NSTATE = 256
NW = 2
NG = 4096
BANDS = 8


def level_of(rng, dims, split, smallest, high):
    gain = 1.0
    for axis_at, blocks in split:
        heights = jax.random.uniform(jax.random.fold_in(jax.random.fold_in(rng, 6), axis_at), (blocks,), jnp.float32, smallest / len(split), high / len(split))
        gain = gain * jnp.repeat(jnp.exp(heights), dims[axis_at] // blocks).reshape((-1,) + (1,) * (len(dims) - 1 - axis_at))
    return gain


def normal_values(key, shape, scale, bound, split=(), dtype=jnp.bfloat16):
    result = scale * jax.random.normal(key, shape, jnp.float32)
    if split:
        result = result * level_of(key, shape, split, -0.22, 0.18)
    return jnp.clip(result, -bound, bound).astype(dtype)


def setup_inputs(seed: int = 0) -> dict:
    arg_keys = jax.random.split(jax.random.key(seed), 7)
    freq_index = jax.random.randint(arg_keys[0], (NW,), 0, 33).astype(jnp.int32)
    band_energy = jnp.clip(jax.random.uniform(arg_keys[1], (BANDS,), jnp.float32, -4.0, 4.0), -4.0, 4.0)
    pole_amp = normal_values(arg_keys[2], (NG, NG), 1.0, 6.0, ((0, 4), (1, 4)), jnp.float32)
    pole_freq = jnp.clip(jnp.exp(math.log(4.0) - 2.0794415 * jax.random.uniform(arg_keys[3], (NG, NG), jnp.float32) ** level_of(arg_keys[3], (NG, NG), ((0, 4), (1, 4)), -0.2, 0.2)), 0.5, 4.0)
    left_pieces = normal_values(arg_keys[4], (BANDS, NSTATE, NG), (1.0 / (NG ** 0.5 * BANDS ** 0.25)), 0.055664062, ((0, 8), (2, 4)))
    right_pieces = normal_values(arg_keys[5], (BANDS, NSTATE, NG), (1.0 / (NG ** 0.5 * BANDS ** 0.25)), 0.055664062, ((0, 8), (2, 4)))
    return dict(freq_index=freq_index, band_energy=band_energy, pole_amp=pole_amp, pole_freq=pole_freq, left_pieces=left_pieces, right_pieces=right_pieces)


def reference(freq_index, band_energy, pole_amp, pole_freq, left_pieces, right_pieces):
    freq = -4.0 + 0.25 * freq_index.astype(jnp.float32)
    nblock = NG // TILE

    def one_band(total, items):
        energy, left_band, right_band = items
        left_blocks = left_band.astype(jnp.float32).reshape(NSTATE, nblock, TILE)
        right_blocks = right_band.astype(jnp.float32).reshape(NSTATE, nblock, TILE)
        results = []
        for w in range(NW):
            distance = freq[w] - energy - pole_freq
            screened = (pole_amp * distance / (distance * distance + 0.25)).astype(jnp.bfloat16)
            blocks = screened.astype(jnp.float32).reshape(nblock, TILE, nblock, TILE)
            partial_value = jnp.einsum("nrg,rgch->nrch", left_blocks, blocks).astype(jnp.bfloat16)
            results.append(jnp.einsum("nrch,mch->nm", partial_value.astype(jnp.float32), right_blocks))
        return total + jnp.stack(results), None

    start = jnp.zeros((NW, NSTATE, NSTATE), jnp.float32)
    sigma, unused = lax.scan(one_band, start, (band_energy, left_pieces, right_pieces))
    return sigma
```

```python
import functools

import jax
import jax.numpy as jnp
from jax import lax
from jax.experimental import pallas as pl
from jax.experimental.pallas import tpu as pltpu
from jax.sharding import PartitionSpec as P

ROWS = 128
SMALL = 16
COLUMNS = 256
VMEM_LIMIT = 12 * 1024 * 1024

WHOLE = pl.BlockSpec(memory_space=pltpu.VMEM)
SCALARS = pl.BlockSpec(memory_space=pltpu.SMEM)


def store_screened(xs, amp_ref, freq_ref, rows, columns, out_ref):
    nfreq = out_ref.shape[1]
    for at in range(0, amp_ref.shape[1], columns):
        here = slice(at, at + columns)
        amp, freq = amp_ref[rows, here], freq_ref[rows, here]
        for n, x in enumerate(xs):
            d = x - freq
            out_ref[n // nfreq, n % nfreq, rows, here] = (amp * d / (d * d + 0.25)).astype(
                jnp.bfloat16
            )


def times_right(s, right):
    return lax.dot_general(
        s, right, (((1,), (1,)), ((), ())), preferred_element_type=jnp.float32
    ).astype(jnp.bfloat16)


def shifts(arrivals, nband, bpiece, places, place_ref, index_ref, energy_ref):
    out = []
    for n in places:
        for k in range(bpiece):
            band = (arrivals(n, place_ref[0]) * nband + place_ref[2]) * bpiece + k
            for w in range(index_ref.shape[0]):
                out.append(-4.0 + 0.25 * index_ref[w].astype(jnp.float32) - energy_ref[band])
    return out


def screen_kernel(
    arrivals,
    nband,
    bpiece,
    place_ref,
    index_ref,
    energy_ref,
    amp_hbm,
    freq_hbm,
    ahead_ref,
    amp_ref,
    freq_ref,
    sems,
):
    steps = sems.shape[0]
    rows = amp_ref.shape[0] // steps

    def copies(i):
        here = pl.ds(pl.multiple_of(i * rows, rows), rows)
        return [
            pltpu.make_async_copy(src.at[here, :], dst.at[here, :], sems.at[i, k])
            for k, (src, dst) in enumerate(((amp_hbm, amp_ref), (freq_hbm, freq_ref)))
        ]

    for i in range(steps):
        for copy in copies(i):
            copy.start()
    xs = shifts(arrivals, nband, bpiece, (0, 1), place_ref, index_ref, energy_ref)

    @pl.loop(0, steps)
    def _(i):
        for copy in copies(i):
            copy.wait()

        @pl.loop(0, rows // SMALL)
        def _(j):
            here = pl.ds(pl.multiple_of(i * rows + j * SMALL, SMALL), SMALL)
            store_screened(xs, amp_ref, freq_ref, here, COLUMNS, ahead_ref)


def screen(place, arrivals, nband, bpiece, freq_index, band_energy, amp, freq):
    g, h = amp.shape
    nfreq = freq_index.shape[0]
    rows = min(ROWS, g)
    held = 8 * g * h + 4 * nfreq * g * bpiece * h
    return pl.pallas_call(
        functools.partial(screen_kernel, arrivals, nband, bpiece),
        in_specs=[SCALARS] * 3 + [pl.BlockSpec(memory_space=pl.ANY)] * 2,
        out_specs=[WHOLE] * 3,
        out_shape=[
            jax.ShapeDtypeStruct((2 * bpiece, nfreq, g, h), jnp.bfloat16),
            jax.ShapeDtypeStruct((g, h), jnp.float32),
            jax.ShapeDtypeStruct((g, h), jnp.float32),
        ],
        scratch_shapes=[pltpu.SemaphoreType.DMA((g // rows, 2))],
        cost_estimate=pl.CostEstimate(
            flops=1024 * bpiece * g * h * nfreq, bytes_accessed=8 * g * h, transcendentals=0
        ),
        compiler_params=pltpu.CompilerParams(vmem_limit_bytes=VMEM_LIMIT + held),
        name="screen",
    )(
        place,
        freq_index,
        band_energy,
        *(pltpu.with_memory_space_constraint(x, pltpu.HBM) for x in (amp, freq)),
    )


def more_kernel(
    arrivals, nband, bpiece, place_ref, index_ref, energy_ref, amp_ref, freq_ref, ahead_ref
):
    places = range(2, 2 + ahead_ref.shape[0] // bpiece)
    xs = shifts(arrivals, nband, bpiece, places, place_ref, index_ref, energy_ref)

    @pl.loop(0, amp_ref.shape[0] // SMALL)
    def _(i):
        here = pl.ds(pl.multiple_of(i * SMALL, SMALL), SMALL)
        store_screened(xs, amp_ref, freq_ref, here, COLUMNS, ahead_ref)


def screen_more(place, arrivals, nband, count, bpiece, freq_index, band_energy, amp, freq):
    g, h = amp.shape
    nfreq = freq_index.shape[0]
    held = 8 * g * h + 2 * nfreq * g * h * count * bpiece
    return pl.pallas_call(
        functools.partial(more_kernel, arrivals, nband, bpiece),
        in_specs=[SCALARS] * 3 + [WHOLE] * 2,
        out_specs=WHOLE,
        out_shape=jax.ShapeDtypeStruct((count * bpiece, nfreq, g, h), jnp.bfloat16),
        cost_estimate=pl.CostEstimate(
            flops=512 * count * bpiece * g * h * nfreq, bytes_accessed=8 * g * h, transcendentals=0
        ),
        compiler_params=pltpu.CompilerParams(vmem_limit_bytes=VMEM_LIMIT + held),
        name="more",
    )(place, freq_index, band_energy, amp, freq)


def apply_kernel(first, ahead_ref, *refs):
    rights, out_ref = refs[:-1], refs[-1]
    for k, right_ref in enumerate(rights):
        nstate = right_ref.shape[0]
        for w in range(ahead_ref.shape[1]):
            out_ref[k, :, w * nstate : (w + 1) * nstate] = times_right(
                ahead_ref[first + k, w], right_ref[...]
            )


def apply_rights(ahead, first, rights):
    count = len(rights)
    _, nfreq, g, h = ahead.shape
    nstate = rights[0].shape[0]
    return pl.pallas_call(
        functools.partial(apply_kernel, first),
        in_specs=[WHOLE] * (count + 1),
        out_specs=WHOLE,
        out_shape=jax.ShapeDtypeStruct((count, g, nfreq * nstate), jnp.bfloat16),
        cost_estimate=pl.CostEstimate(
            flops=2 * count * g * h * nfreq * nstate,
            bytes_accessed=2 * count * nfreq * g * h,
            transcendentals=0,
        ),
        compiler_params=pltpu.CompilerParams(vmem_limit_bytes=VMEM_LIMIT + 2 * ahead.size),
        name="apply",
    )(ahead, *rights)


def fold_kernel(slots, ntables, has_init, place_ref, *rest):
    count = len(slots)
    lefts = rest[:count]
    tables = rest[count : count + ntables]
    out_ref, acc = rest[-2], rest[-1]
    acc[...] = rest[-3][...] if has_init else jnp.zeros_like(acc)
    here = [place_ref[i] for i in range(3)]
    for left_ref, (slot_of, use_of, k) in zip(lefts, slots):
        slot = slot_of(*here)
        for at, table_ref in enumerate(tables):
            chosen = slot == at if use_of is None else (slot == at) & use_of(*here)

            @pl.when(chosen)
            def _():
                acc[...] += jnp.dot(
                    left_ref[...], table_ref[k], preferred_element_type=jnp.float32
                )

    out_ref[...] = acc[...].astype(out_ref.dtype)


def fold(place, pieces, tables, init, nstate, dtype):
    lefts, slots = zip(*pieces)
    g, width = tables[0].shape[1:]
    args = [place, *lefts, *tables]
    if init is not None:
        args.append(init)
    return pl.pallas_call(
        functools.partial(fold_kernel, slots, len(tables), init is not None),
        in_specs=[SCALARS] + [WHOLE] * (len(args) - 1),
        out_specs=WHOLE,
        scratch_shapes=[pltpu.VMEM((nstate, width), jnp.float32)],
        out_shape=jax.ShapeDtypeStruct((nstate, width), dtype),
        cost_estimate=pl.CostEstimate(
            flops=2 * len(lefts) * nstate * g * width,
            bytes_accessed=2 * len(lefts) * g * (width + nstate),
            transcendentals=0,
        ),
        compiler_params=pltpu.CompilerParams(vmem_limit_bytes=VMEM_LIMIT),
        name="fold",
    )(*args)


def xor_pairs(n, d):
    return [(i, i ^ d) for i in range(n)]


def gather_xor(piece, axis):
    n = lax.axis_size(axis)
    if n & (n - 1):
        me = lax.axis_index(axis)
        every = lax.all_gather(piece, axis, axis=0)
        return [
            lax.dynamic_index_in_dim(every, (me + d) % n, 0, False) for d in range(n)
        ], lambda d, me: (me + d) % n
    found = [piece] + [lax.ppermute(piece, axis, xor_pairs(n, d)) for d in range(1, n)]
    return found, lambda d, me: d ^ me


def is_line(ncol):
    return ncol == 4


def body(freq_index, band_energy, pole_amp, pole_freq, left_pieces, right_pieces):
    bpiece, nstate = left_pieces.shape[:2]
    nfreq = freq_index.shape[0]
    nband, nrow, ncol = (lax.axis_size(a) for a in ("band", "row", "col"))
    axes = ("row", "col", "band")
    line = is_line(ncol)
    place = jnp.stack([lax.axis_index(a) for a in axes]).astype(jnp.int32)

    rights, whose = gather_xor(right_pieces, "row")
    if nrow & (nrow - 1):
        table_of = lambda q, row: (q + nrow - row) % nrow
    else:
        table_of = lambda q, row: q ^ row

    def pieces(left, owner, use=None):
        slot = lambda row, col, group: table_of(owner(col), row)
        return [(left[k], (slot, use, k)) for k in range(bpiece)]

    if line:
        far = lax.ppermute(left_pieces, "col", xor_pairs(4, 2))
        near = lax.ppermute(left_pieces, "col", xor_pairs(4, 1))
        mid = lax.ppermute(left_pieces, "col", [(1, 2), (2, 1)])
        hop = lax.ppermute(far, "col", [(2, 3), (1, 0)])
        inner = lambda row, col, group: (col == 1) | (col == 2)
        outer = lambda row, col, group: (col == 0) | (col == 3)
        soon = (
            pieces(left_pieces, lambda col: col)
            + pieces(near, lambda col: col ^ 1)
            + pieces(far, lambda col: col ^ 2)
        )
        last = pieces(mid, lambda col: col ^ 3, inner) + pieces(hop, lambda col: col ^ 3, outer)
    else:
        lefts, owner_of = gather_xor(left_pieces, "col")
        last = [
            p
            for d, left in enumerate(lefts)
            for p in pieces(left, lambda col, d=d: owner_of(d, col))
        ]

    scalars = freq_index, band_energy
    ahead, amp, freq = screen(place, whose, nband, bpiece, *scalars, pole_amp, pole_freq)
    later = screen_more(place, whose, nband, nrow - 2, bpiece, *scalars, amp, freq)
    tables = []
    for d in range(nrow):
        source, first = (ahead, d) if d < 2 else (later, d - 2)
        held = [rights[d][k] for k in range(bpiece)]
        tables.append(apply_rights(source, first * bpiece, held))

    total = None
    if line:
        total = fold(place, soon, tables, None, nstate, jnp.float32)
    total = fold(place, last, tables, total, nstate, jnp.bfloat16)
    parts = lax.all_to_all(total, axes, split_axis=0, concat_axis=0, tiled=True)
    ndev = lax.axis_size(axes)
    owned = nstate // ndev
    mine = jnp.sum(parts.reshape(ndev, owned, nfreq, nstate).astype(jnp.float32), axis=0)
    return mine.transpose(1, 0, 2)


def solution(mesh):
    in_specs = (
        P(),
        P(),
        P("row", "col"),
        P("row", "col"),
        P(("col", "band"), None, "row"),
        P(("row", "band"), None, "col"),
    )
    out_specs = P(None, ("row", "col", "band"), None)

    return jax.shard_map(body, mesh=mesh, in_specs=in_specs, out_specs=out_specs, check_vma=False)
```

```python
import functools

import jax
import jax.numpy as jnp
from jax import lax
from jax.experimental import pallas as pl
from jax.experimental.pallas import tpu as pltpu
from jax.sharding import PartitionSpec as P

ROWS = 128
SMALL = 16
COLUMNS = 256
VMEM_LIMIT = 12 * 1024 * 1024

WHOLE = pl.BlockSpec(memory_space=pltpu.VMEM)
SCALARS = pl.BlockSpec(memory_space=pltpu.SMEM)


def store_screened(xs, amp_ref, freq_ref, rows, columns, out_ref):
    nfreq = out_ref.shape[1]
    for at in range(0, amp_ref.shape[1], columns):
        here = slice(at, at + columns)
        amp, freq = amp_ref[rows, here], freq_ref[rows, here]
        for n, x in enumerate(xs):
            d = x - freq
            out_ref[n // nfreq, n % nfreq, rows, here] = (amp * d / (d * d + 0.25)).astype(
                jnp.bfloat16
            )


def times_right(s, right):
    return lax.dot_general(
        s, right, (((1,), (1,)), ((), ())), preferred_element_type=jnp.float32
    ).astype(jnp.bfloat16)


def shifts(arrivals, nband, bpiece, places, place_ref, index_ref, energy_ref):
    out = []
    for n in places:
        for k in range(bpiece):
            band = (arrivals(n, place_ref[0]) * nband + place_ref[2]) * bpiece + k
            for w in range(index_ref.shape[0]):
                out.append(-4.0 + 0.25 * index_ref[w].astype(jnp.float32) - energy_ref[band])
    return out


def screen_kernel(
    arrivals,
    nband,
    bpiece,
    place_ref,
    index_ref,
    energy_ref,
    amp_hbm,
    freq_hbm,
    ahead_ref,
    amp_ref,
    freq_ref,
    sems,
):
    steps = sems.shape[0]
    rows = amp_ref.shape[0] // steps

    def copies(i):
        here = pl.ds(pl.multiple_of(i * rows, rows), rows)
        return [
            pltpu.make_async_copy(src.at[here, :], dst.at[here, :], sems.at[i, k])
            for k, (src, dst) in enumerate(((amp_hbm, amp_ref), (freq_hbm, freq_ref)))
        ]

    for i in range(steps):
        for copy in copies(i):
            copy.start()
    xs = shifts(arrivals, nband, bpiece, (0, 1), place_ref, index_ref, energy_ref)

    @pl.loop(0, steps)
    def _(i):
        for copy in copies(i):
            copy.wait()

        @pl.loop(0, rows // SMALL)
        def _(j):
            here = pl.ds(pl.multiple_of(i * rows + j * SMALL, SMALL), SMALL)
            store_screened(xs, amp_ref, freq_ref, here, COLUMNS, ahead_ref)


def screen(place, arrivals, nband, bpiece, freq_index, band_energy, amp, freq):
    g, h = amp.shape
    nfreq = freq_index.shape[0]
    rows = min(ROWS, g)
    held = 8 * g * h + 4 * nfreq * g * bpiece * h
    return pl.pallas_call(
        functools.partial(screen_kernel, arrivals, nband, bpiece),
        in_specs=[SCALARS] * 3 + [pl.BlockSpec(memory_space=pl.ANY)] * 2,
        out_specs=[WHOLE] * 3,
        out_shape=[
            jax.ShapeDtypeStruct((2 * bpiece, nfreq, g, h), jnp.bfloat16),
            jax.ShapeDtypeStruct((g, h), jnp.float32),
            jax.ShapeDtypeStruct((g, h), jnp.float32),
        ],
        scratch_shapes=[pltpu.SemaphoreType.DMA((g // rows, 2))],
        cost_estimate=pl.CostEstimate(
            flops=1024 * bpiece * g * h * nfreq, bytes_accessed=8 * g * h, transcendentals=0
        ),
        compiler_params=pltpu.CompilerParams(vmem_limit_bytes=VMEM_LIMIT + held),
        name="screen",
    )(
        place,
        freq_index,
        band_energy,
        *(pltpu.with_memory_space_constraint(x, pltpu.HBM) for x in (amp, freq)),
    )


def more_kernel(
    arrivals, nband, bpiece, place_ref, index_ref, energy_ref, amp_ref, freq_ref, ahead_ref
):
    places = range(2, 2 + ahead_ref.shape[0] // bpiece)
    xs = shifts(arrivals, nband, bpiece, places, place_ref, index_ref, energy_ref)

    @pl.loop(0, amp_ref.shape[0] // SMALL)
    def _(i):
        here = pl.ds(pl.multiple_of(i * SMALL, SMALL), SMALL)
        store_screened(xs, amp_ref, freq_ref, here, COLUMNS, ahead_ref)


def screen_more(place, arrivals, nband, count, bpiece, freq_index, band_energy, amp, freq):
    g, h = amp.shape
    nfreq = freq_index.shape[0]
    held = 8 * g * h + 2 * nfreq * g * h * count * bpiece
    return pl.pallas_call(
        functools.partial(more_kernel, arrivals, nband, bpiece),
        in_specs=[SCALARS] * 3 + [WHOLE] * 2,
        out_specs=WHOLE,
        out_shape=jax.ShapeDtypeStruct((count * bpiece, nfreq, g, h), jnp.bfloat16),
        cost_estimate=pl.CostEstimate(
            flops=512 * count * bpiece * g * h * nfreq, bytes_accessed=8 * g * h, transcendentals=0
        ),
        compiler_params=pltpu.CompilerParams(vmem_limit_bytes=VMEM_LIMIT + held),
        name="more",
    )(place, freq_index, band_energy, amp, freq)


def apply_kernel(first, ahead_ref, *refs):
    rights, out_ref = refs[:-1], refs[-1]
    for k, right_ref in enumerate(rights):
        nstate = right_ref.shape[0]
        for w in range(ahead_ref.shape[1]):
            out_ref[k, :, w * nstate : (w + 1) * nstate] = times_right(
                ahead_ref[first + k, w], right_ref[...]
            )


def apply_rights(ahead, first, rights):
    count = len(rights)
    _, nfreq, g, h = ahead.shape
    nstate = rights[0].shape[0]
    return pl.pallas_call(
        functools.partial(apply_kernel, first),
        in_specs=[WHOLE] * (count + 1),
        out_specs=WHOLE,
        out_shape=jax.ShapeDtypeStruct((count, g, nfreq * nstate), jnp.bfloat16),
        cost_estimate=pl.CostEstimate(
            flops=2 * count * g * h * nfreq * nstate,
            bytes_accessed=2 * count * nfreq * g * h,
            transcendentals=0,
        ),
        compiler_params=pltpu.CompilerParams(vmem_limit_bytes=VMEM_LIMIT + 2 * ahead.size),
        name="apply",
    )(ahead, *rights)


def fold_kernel(slots, ntables, has_init, place_ref, *rest):
    count = len(slots)
    lefts = rest[:count]
    tables = rest[count : count + ntables]
    out_ref, acc = rest[-2], rest[-1]
    acc[...] = rest[-3][...] if has_init else jnp.zeros_like(acc)
    here = [place_ref[i] for i in range(3)]
    for left_ref, (slot_of, use_of, k) in zip(lefts, slots):
        slot = slot_of(*here)
        for at, table_ref in enumerate(tables):
            chosen = slot == at if use_of is None else (slot == at) & use_of(*here)

            @pl.when(chosen)
            def _():
                acc[...] += jnp.dot(
                    left_ref[...], table_ref[k], preferred_element_type=jnp.float32
                )

    out_ref[...] = acc[...].astype(out_ref.dtype)


def fold(place, pieces, tables, init, nstate, dtype):
    lefts, slots = zip(*pieces)
    g, width = tables[0].shape[1:]
    args = [place, *lefts, *tables]
    if init is not None:
        args.append(init)
    return pl.pallas_call(
        functools.partial(fold_kernel, slots, len(tables), init is not None),
        in_specs=[SCALARS] + [WHOLE] * (len(args) - 1),
        out_specs=WHOLE,
        scratch_shapes=[pltpu.VMEM((nstate, width), jnp.float32)],
        out_shape=jax.ShapeDtypeStruct((nstate, width), dtype),
        cost_estimate=pl.CostEstimate(
            flops=2 * len(lefts) * nstate * g * width,
            bytes_accessed=2 * len(lefts) * g * (width + nstate),
            transcendentals=0,
        ),
        compiler_params=pltpu.CompilerParams(vmem_limit_bytes=VMEM_LIMIT),
        name="fold",
    )(*args)


def xor_pairs(n, d):
    return [(i, i ^ d) for i in range(n)]


def gather_xor(piece, axis):
    n = lax.axis_size(axis)
    if n & (n - 1):
        me = lax.axis_index(axis)
        every = lax.all_gather(piece, axis, axis=0)
        return [
            lax.dynamic_index_in_dim(every, (me + d) % n, 0, False) for d in range(n)
        ], lambda d, me: (me + d) % n
    found = [piece] + [lax.ppermute(piece, axis, xor_pairs(n, d)) for d in range(1, n)]
    return found, lambda d, me: d ^ me


def is_line(ncol):
    return ncol == 4


def body(freq_index, band_energy, pole_amp, pole_freq, left_pieces, right_pieces):
    bpiece, nstate = left_pieces.shape[:2]
    nfreq = freq_index.shape[0]
    nband, nrow, ncol = (lax.axis_size(a) for a in ("band", "row", "col"))
    axes = ("row", "col", "band")
    line = is_line(ncol)
    place = jnp.stack([lax.axis_index(a) for a in axes]).astype(jnp.int32)

    rights, whose = gather_xor(right_pieces, "row")
    if nrow & (nrow - 1):
        table_of = lambda q, row: (q + nrow - row) % nrow
    else:
        table_of = lambda q, row: q ^ row

    def pieces(left, owner, use=None):
        slot = lambda row, col, group: table_of(owner(col), row)
        return [(left[k], (slot, use, k)) for k in range(bpiece)]

    if line:
        inward = lax.ppermute(left_pieces, "col", [(0, 2), (3, 1)])
        outward = lax.ppermute(left_pieces, "col", [(1, 3), (2, 0)])
        near = lax.ppermute(left_pieces, "col", xor_pairs(4, 1))
        mid = lax.ppermute(left_pieces, "col", [(1, 2), (2, 1)])
        hop = lax.ppermute(inward, "col", [(2, 3), (1, 0)])
        inner = lambda row, col, group: (col == 1) | (col == 2)
        outer = lambda row, col, group: (col == 0) | (col == 3)
        soon = (
            pieces(left_pieces, lambda col: col)
            + pieces(near, lambda col: col ^ 1)
            + pieces(inward, lambda col: col ^ 2, inner)
            + pieces(outward, lambda col: col ^ 2, outer)
        )
        last = pieces(mid, lambda col: col ^ 3, inner) + pieces(hop, lambda col: col ^ 3, outer)
    else:
        lefts, owner_of = gather_xor(left_pieces, "col")
        last = [
            p
            for d, left in enumerate(lefts)
            for p in pieces(left, lambda col, d=d: owner_of(d, col))
        ]

    scalars = freq_index, band_energy
    ahead, amp, freq = screen(place, whose, nband, bpiece, *scalars, pole_amp, pole_freq)
    later = screen_more(place, whose, nband, nrow - 2, bpiece, *scalars, amp, freq)
    tables = []
    for d in range(nrow):
        source, first = (ahead, d) if d < 2 else (later, d - 2)
        held = [rights[d][k] for k in range(bpiece)]
        tables.append(apply_rights(source, first * bpiece, held))

    total = None
    if line:
        total = fold(place, soon, tables, None, nstate, jnp.float32)
    total = fold(place, last, tables, total, nstate, jnp.bfloat16)
    parts = lax.all_to_all(total, axes, split_axis=0, concat_axis=0, tiled=True)
    ndev = lax.axis_size(axes)
    owned = nstate // ndev
    mine = jnp.sum(parts.reshape(ndev, owned, nfreq, nstate).astype(jnp.float32), axis=0)
    return mine.transpose(1, 0, 2)


def solution(mesh):
    in_specs = (
        P(),
        P(),
        P("row", "col"),
        P("row", "col"),
        P(("col", "band"), None, "row"),
        P(("row", "band"), None, "col"),
    )
    out_specs = P(None, ("row", "col", "band"), None)

    return jax.shard_map(body, mesh=mesh, in_specs=in_specs, out_specs=out_specs, check_vma=False)
```

```python
import functools

import jax
import jax.numpy as jnp
from jax import lax
from jax.experimental import pallas as pl
from jax.experimental.pallas import tpu as pltpu
from jax.sharding import PartitionSpec as P

ROWS = 128
SMALL = 16
COLUMNS = 256
VMEM_LIMIT = 12 * 1024 * 1024

WHOLE = pl.BlockSpec(memory_space=pltpu.VMEM)
SCALARS = pl.BlockSpec(memory_space=pltpu.SMEM)


def store_screened(xs, amp_ref, freq_ref, rows, columns, out_ref):
    nfreq = out_ref.shape[1]
    for at in range(0, amp_ref.shape[1], columns):
        here = slice(at, at + columns)
        amp, freq = amp_ref[rows, here], freq_ref[rows, here]
        for n, x in enumerate(xs):
            d = x - freq
            out_ref[n // nfreq, n % nfreq, rows, here] = (amp * d / (d * d + 0.25)).astype(
                jnp.bfloat16
            )


def times_right(s, right):
    return lax.dot_general(
        s, right, (((1,), (1,)), ((), ())), preferred_element_type=jnp.float32
    ).astype(jnp.bfloat16)


def shifts(arrivals, nband, bpiece, places, place_ref, index_ref, energy_ref):
    out = []
    for n in places:
        for k in range(bpiece):
            band = (arrivals(n, place_ref[0]) * nband + place_ref[2]) * bpiece + k
            for w in range(index_ref.shape[0]):
                out.append(-4.0 + 0.25 * index_ref[w].astype(jnp.float32) - energy_ref[band])
    return out


def screen_kernel(
    arrivals,
    nband,
    bpiece,
    place_ref,
    index_ref,
    energy_ref,
    amp_hbm,
    freq_hbm,
    ahead_ref,
    amp_ref,
    freq_ref,
    sems,
):
    steps = sems.shape[0]
    rows = amp_ref.shape[0] // steps

    def copies(i):
        here = pl.ds(pl.multiple_of(i * rows, rows), rows)
        return [
            pltpu.make_async_copy(src.at[here, :], dst.at[here, :], sems.at[i, k])
            for k, (src, dst) in enumerate(((amp_hbm, amp_ref), (freq_hbm, freq_ref)))
        ]

    for i in range(steps):
        for copy in copies(i):
            copy.start()
    xs = shifts(arrivals, nband, bpiece, (0, 1), place_ref, index_ref, energy_ref)

    @pl.loop(0, steps)
    def _(i):
        for copy in copies(i):
            copy.wait()

        @pl.loop(0, rows // SMALL)
        def _(j):
            here = pl.ds(pl.multiple_of(i * rows + j * SMALL, SMALL), SMALL)
            store_screened(xs, amp_ref, freq_ref, here, COLUMNS, ahead_ref)


def screen(place, arrivals, nband, bpiece, freq_index, band_energy, amp, freq):
    g, h = amp.shape
    nfreq = freq_index.shape[0]
    rows = min(ROWS, g)
    held = 8 * g * h + 4 * nfreq * g * bpiece * h
    return pl.pallas_call(
        functools.partial(screen_kernel, arrivals, nband, bpiece),
        in_specs=[SCALARS] * 3 + [pl.BlockSpec(memory_space=pl.ANY)] * 2,
        out_specs=[WHOLE] * 3,
        out_shape=[
            jax.ShapeDtypeStruct((2 * bpiece, nfreq, g, h), jnp.bfloat16),
            jax.ShapeDtypeStruct((g, h), jnp.float32),
            jax.ShapeDtypeStruct((g, h), jnp.float32),
        ],
        scratch_shapes=[pltpu.SemaphoreType.DMA((g // rows, 2))],
        cost_estimate=pl.CostEstimate(
            flops=1024 * bpiece * g * h * nfreq, bytes_accessed=8 * g * h, transcendentals=0
        ),
        compiler_params=pltpu.CompilerParams(vmem_limit_bytes=VMEM_LIMIT + held),
        name="screen",
    )(
        place,
        freq_index,
        band_energy,
        *(pltpu.with_memory_space_constraint(x, pltpu.HBM) for x in (amp, freq)),
    )


def more_kernel(
    arrivals, nband, bpiece, place_ref, index_ref, energy_ref, amp_ref, freq_ref, ahead_ref
):
    places = range(2, 2 + ahead_ref.shape[0] // bpiece)
    xs = shifts(arrivals, nband, bpiece, places, place_ref, index_ref, energy_ref)

    @pl.loop(0, amp_ref.shape[0] // SMALL)
    def _(i):
        here = pl.ds(pl.multiple_of(i * SMALL, SMALL), SMALL)
        store_screened(xs, amp_ref, freq_ref, here, COLUMNS, ahead_ref)


def screen_more(place, arrivals, nband, count, bpiece, freq_index, band_energy, amp, freq):
    g, h = amp.shape
    nfreq = freq_index.shape[0]
    held = 8 * g * h + 2 * nfreq * g * h * count * bpiece
    return pl.pallas_call(
        functools.partial(more_kernel, arrivals, nband, bpiece),
        in_specs=[SCALARS] * 3 + [WHOLE] * 2,
        out_specs=WHOLE,
        out_shape=jax.ShapeDtypeStruct((count * bpiece, nfreq, g, h), jnp.bfloat16),
        cost_estimate=pl.CostEstimate(
            flops=512 * count * bpiece * g * h * nfreq, bytes_accessed=8 * g * h, transcendentals=0
        ),
        compiler_params=pltpu.CompilerParams(vmem_limit_bytes=VMEM_LIMIT + held),
        name="more",
    )(place, freq_index, band_energy, amp, freq)


def apply_kernel(first, ahead_ref, *refs):
    rights, out_ref = refs[:-1], refs[-1]
    for k, right_ref in enumerate(rights):
        nstate = right_ref.shape[0]
        for w in range(ahead_ref.shape[1]):
            out_ref[k, :, w * nstate : (w + 1) * nstate] = times_right(
                ahead_ref[first + k, w], right_ref[...]
            )


def apply_rights(ahead, first, rights):
    count = len(rights)
    _, nfreq, g, h = ahead.shape
    nstate = rights[0].shape[0]
    return pl.pallas_call(
        functools.partial(apply_kernel, first),
        in_specs=[WHOLE] * (count + 1),
        out_specs=WHOLE,
        out_shape=jax.ShapeDtypeStruct((count, g, nfreq * nstate), jnp.bfloat16),
        cost_estimate=pl.CostEstimate(
            flops=2 * count * g * h * nfreq * nstate,
            bytes_accessed=2 * count * nfreq * g * h,
            transcendentals=0,
        ),
        compiler_params=pltpu.CompilerParams(vmem_limit_bytes=VMEM_LIMIT + 2 * ahead.size),
        name="apply",
    )(ahead, *rights)


def fold_kernel(slots, ntables, has_init, *rest):
    count = len(slots)
    lefts = rest[:count]
    tables = rest[count : count + ntables]
    out_ref, acc = rest[-2], rest[-1]
    acc[...] = rest[-3][...] if has_init else jnp.zeros_like(acc)
    here = [lax.axis_index(a) for a in ("row", "col", "band")]
    for left_ref, (slot_of, use_of, k) in zip(lefts, slots):
        slot = slot_of(*here)
        for at, table_ref in enumerate(tables):
            chosen = slot == at if use_of is None else (slot == at) & use_of(*here)

            @pl.when(chosen)
            def _():
                acc[...] += jnp.dot(
                    left_ref[...], table_ref[k], preferred_element_type=jnp.float32
                )

    out_ref[...] = acc[...].astype(out_ref.dtype)


def fold(pieces, tables, init, nstate, dtype):
    lefts, slots = zip(*pieces)
    g, width = tables[0].shape[1:]
    args = [*lefts, *tables]
    if init is not None:
        args.append(init)
    return pl.pallas_call(
        functools.partial(fold_kernel, slots, len(tables), init is not None),
        in_specs=[WHOLE] * len(args),
        out_specs=WHOLE,
        scratch_shapes=[pltpu.VMEM((nstate, width), jnp.float32)],
        out_shape=jax.ShapeDtypeStruct((nstate, width), dtype),
        cost_estimate=pl.CostEstimate(
            flops=2 * len(lefts) * nstate * g * width,
            bytes_accessed=2 * len(lefts) * g * (width + nstate),
            transcendentals=0,
        ),
        compiler_params=pltpu.CompilerParams(vmem_limit_bytes=VMEM_LIMIT),
        name="fold",
    )(*args)


def xor_pairs(n, d):
    return [(i, i ^ d) for i in range(n)]


def gather_xor(piece, axis):
    n = lax.axis_size(axis)
    if n & (n - 1):
        me = lax.axis_index(axis)
        every = lax.all_gather(piece, axis, axis=0)
        return [
            lax.dynamic_index_in_dim(every, (me + d) % n, 0, False) for d in range(n)
        ], lambda d, me: (me + d) % n
    found = [piece] + [lax.ppermute(piece, axis, xor_pairs(n, d)) for d in range(1, n)]
    return found, lambda d, me: d ^ me


def is_line(ncol):
    return ncol == 4


def body(freq_index, band_energy, pole_amp, pole_freq, left_pieces, right_pieces):
    bpiece, nstate = left_pieces.shape[:2]
    nfreq = freq_index.shape[0]
    nband, nrow, ncol = (lax.axis_size(a) for a in ("band", "row", "col"))
    axes = ("row", "col", "band")
    line = is_line(ncol)
    place = jnp.stack([lax.axis_index(a) for a in axes]).astype(jnp.int32)

    rights, whose = gather_xor(right_pieces, "row")
    if nrow & (nrow - 1):
        table_of = lambda q, row: (q + nrow - row) % nrow
    else:
        table_of = lambda q, row: q ^ row

    def pieces(left, owner, use=None):
        slot = lambda row, col, group: table_of(owner(col), row)
        return [(left[k], (slot, use, k)) for k in range(bpiece)]

    if line:
        inward = lax.ppermute(left_pieces, "col", [(0, 2), (3, 1)])
        outward = lax.ppermute(left_pieces, "col", [(1, 3), (2, 0)])
        near = lax.ppermute(left_pieces, "col", xor_pairs(4, 1))
        mid = lax.ppermute(left_pieces, "col", [(1, 2), (2, 1)])
        hop = lax.ppermute(inward, "col", [(2, 3), (1, 0)])
        inner = lambda row, col, group: (col == 1) | (col == 2)
        outer = lambda row, col, group: (col == 0) | (col == 3)
        soon = (
            pieces(left_pieces, lambda col: col)
            + pieces(near, lambda col: col ^ 1)
            + pieces(inward, lambda col: col ^ 2, inner)
            + pieces(outward, lambda col: col ^ 2, outer)
        )
        last = pieces(mid, lambda col: col ^ 3, inner) + pieces(hop, lambda col: col ^ 3, outer)
    else:
        lefts, owner_of = gather_xor(left_pieces, "col")
        last = [
            p
            for d, left in enumerate(lefts)
            for p in pieces(left, lambda col, d=d: owner_of(d, col))
        ]

    scalars = freq_index, band_energy
    ahead, amp, freq = screen(place, whose, nband, bpiece, *scalars, pole_amp, pole_freq)
    later = screen_more(place, whose, nband, nrow - 2, bpiece, *scalars, amp, freq)
    tables = []
    for d in range(nrow):
        source, first = (ahead, d) if d < 2 else (later, d - 2)
        held = [rights[d][k] for k in range(bpiece)]
        tables.append(apply_rights(source, first * bpiece, held))

    total = None
    if line:
        total = fold(soon, tables, None, nstate, jnp.float32)
    total = fold(last, tables, total, nstate, jnp.bfloat16)
    parts = lax.all_to_all(total, axes, split_axis=0, concat_axis=0, tiled=True)
    ndev = lax.axis_size(axes)
    owned = nstate // ndev
    mine = jnp.sum(parts.reshape(ndev, owned, nfreq, nstate).astype(jnp.float32), axis=0)
    return mine.transpose(1, 0, 2)


def solution(mesh):
    in_specs = (
        P(),
        P(),
        P("row", "col"),
        P("row", "col"),
        P(("col", "band"), None, "row"),
        P(("row", "band"), None, "col"),
    )
    out_specs = P(None, ("row", "col", "band"), None)

    return jax.shard_map(body, mesh=mesh, in_specs=in_specs, out_specs=out_specs, check_vma=False)
```

```python
import functools

import jax
import jax.numpy as jnp
from jax import lax
from jax.experimental import pallas as pl
from jax.experimental.pallas import tpu as pltpu
from jax.sharding import PartitionSpec as P

ROWS = 128
SMALL = 16
COLUMNS = 256
VMEM_LIMIT = 12 * 1024 * 1024

WHOLE = pl.BlockSpec(memory_space=pltpu.VMEM)
SCALARS = pl.BlockSpec(memory_space=pltpu.SMEM)


def store_screened(xs, amp_ref, freq_ref, rows, columns, out_ref):
    nfreq = out_ref.shape[1]
    for at in range(0, amp_ref.shape[1], columns):
        here = slice(at, at + columns)
        amp, freq = amp_ref[rows, here], freq_ref[rows, here]
        for n, x in enumerate(xs):
            d = x - freq
            out_ref[n // nfreq, n % nfreq, rows, here] = (amp * d / (d * d + 0.25)).astype(
                jnp.bfloat16
            )


def times_right(s, right):
    return lax.dot_general(
        s, right, (((1,), (1,)), ((), ())), preferred_element_type=jnp.float32
    ).astype(jnp.bfloat16)


def shifts(arrivals, nband, bpiece, places, index_ref, energy_ref):
    row, group = lax.axis_index("row"), lax.axis_index("band")
    out = []
    for n in places:
        for k in range(bpiece):
            band = (arrivals(n, row) * nband + group) * bpiece + k
            for w in range(index_ref.shape[0]):
                out.append(-4.0 + 0.25 * index_ref[w].astype(jnp.float32) - energy_ref[band])
    return out


def screen_kernel(
    arrivals,
    nband,
    bpiece,
    index_ref,
    energy_ref,
    amp_hbm,
    freq_hbm,
    ahead_ref,
    amp_ref,
    freq_ref,
    sems,
):
    steps = sems.shape[0]
    rows = amp_ref.shape[0] // steps

    def copies(i):
        here = pl.ds(pl.multiple_of(i * rows, rows), rows)
        return [
            pltpu.make_async_copy(src.at[here, :], dst.at[here, :], sems.at[i, k])
            for k, (src, dst) in enumerate(((amp_hbm, amp_ref), (freq_hbm, freq_ref)))
        ]

    for i in range(steps):
        for copy in copies(i):
            copy.start()
    xs = shifts(arrivals, nband, bpiece, (0, 1), index_ref, energy_ref)

    @pl.loop(0, steps)
    def _(i):
        for copy in copies(i):
            copy.wait()

        @pl.loop(0, rows // SMALL)
        def _(j):
            here = pl.ds(pl.multiple_of(i * rows + j * SMALL, SMALL), SMALL)
            store_screened(xs, amp_ref, freq_ref, here, COLUMNS, ahead_ref)


def screen(arrivals, nband, bpiece, freq_index, band_energy, amp, freq):
    g, h = amp.shape
    nfreq = freq_index.shape[0]
    rows = min(ROWS, g)
    held = 8 * g * h + 4 * nfreq * g * bpiece * h
    return pl.pallas_call(
        functools.partial(screen_kernel, arrivals, nband, bpiece),
        in_specs=[SCALARS] * 2 + [pl.BlockSpec(memory_space=pl.ANY)] * 2,
        out_specs=[WHOLE] * 3,
        out_shape=[
            jax.ShapeDtypeStruct((2 * bpiece, nfreq, g, h), jnp.bfloat16),
            jax.ShapeDtypeStruct((g, h), jnp.float32),
            jax.ShapeDtypeStruct((g, h), jnp.float32),
        ],
        scratch_shapes=[pltpu.SemaphoreType.DMA((g // rows, 2))],
        cost_estimate=pl.CostEstimate(
            flops=1024 * bpiece * g * h * nfreq, bytes_accessed=8 * g * h, transcendentals=0
        ),
        compiler_params=pltpu.CompilerParams(vmem_limit_bytes=VMEM_LIMIT + held),
        name="screen",
    )(
        freq_index,
        band_energy,
        *(pltpu.with_memory_space_constraint(x, pltpu.HBM) for x in (amp, freq)),
    )


def more_kernel(
    arrivals, nband, bpiece, index_ref, energy_ref, amp_ref, freq_ref, ahead_ref
):
    places = range(2, 2 + ahead_ref.shape[0] // bpiece)
    xs = shifts(arrivals, nband, bpiece, places, index_ref, energy_ref)

    @pl.loop(0, amp_ref.shape[0] // SMALL)
    def _(i):
        here = pl.ds(pl.multiple_of(i * SMALL, SMALL), SMALL)
        store_screened(xs, amp_ref, freq_ref, here, COLUMNS, ahead_ref)


def screen_more(arrivals, nband, count, bpiece, freq_index, band_energy, amp, freq):
    g, h = amp.shape
    nfreq = freq_index.shape[0]
    held = 8 * g * h + 2 * nfreq * g * h * count * bpiece
    return pl.pallas_call(
        functools.partial(more_kernel, arrivals, nband, bpiece),
        in_specs=[SCALARS] * 2 + [WHOLE] * 2,
        out_specs=WHOLE,
        out_shape=jax.ShapeDtypeStruct((count * bpiece, nfreq, g, h), jnp.bfloat16),
        cost_estimate=pl.CostEstimate(
            flops=512 * count * bpiece * g * h * nfreq, bytes_accessed=8 * g * h, transcendentals=0
        ),
        compiler_params=pltpu.CompilerParams(vmem_limit_bytes=VMEM_LIMIT + held),
        name="more",
    )(freq_index, band_energy, amp, freq)


def apply_kernel(first, ahead_ref, *refs):
    rights, out_ref = refs[:-1], refs[-1]
    for k, right_ref in enumerate(rights):
        nstate = right_ref.shape[0]
        for w in range(ahead_ref.shape[1]):
            out_ref[k, :, w * nstate : (w + 1) * nstate] = times_right(
                ahead_ref[first + k, w], right_ref[...]
            )


def apply_rights(ahead, first, rights):
    count = len(rights)
    _, nfreq, g, h = ahead.shape
    nstate = rights[0].shape[0]
    return pl.pallas_call(
        functools.partial(apply_kernel, first),
        in_specs=[WHOLE] * (count + 1),
        out_specs=WHOLE,
        out_shape=jax.ShapeDtypeStruct((count, g, nfreq * nstate), jnp.bfloat16),
        cost_estimate=pl.CostEstimate(
            flops=2 * count * g * h * nfreq * nstate,
            bytes_accessed=2 * count * nfreq * g * h,
            transcendentals=0,
        ),
        compiler_params=pltpu.CompilerParams(vmem_limit_bytes=VMEM_LIMIT + 2 * ahead.size),
        name="apply",
    )(ahead, *rights)


def fold_kernel(slots, ntables, has_init, *rest):
    count = len(slots)
    lefts = rest[:count]
    tables = rest[count : count + ntables]
    out_ref, acc = rest[-2], rest[-1]
    acc[...] = rest[-3][...] if has_init else jnp.zeros_like(acc)
    here = [lax.axis_index(a) for a in ("row", "col", "band")]
    for left_ref, (slot_of, use_of, k) in zip(lefts, slots):
        slot = slot_of(*here)
        for at, table_ref in enumerate(tables):
            chosen = slot == at if use_of is None else (slot == at) & use_of(*here)

            @pl.when(chosen)
            def _():
                acc[...] += jnp.dot(
                    left_ref[...], table_ref[k], preferred_element_type=jnp.float32
                )

    out_ref[...] = acc[...].astype(out_ref.dtype)


def fold(pieces, tables, init, nstate, dtype):
    lefts, slots = zip(*pieces)
    g, width = tables[0].shape[1:]
    args = [*lefts, *tables]
    if init is not None:
        args.append(init)
    return pl.pallas_call(
        functools.partial(fold_kernel, slots, len(tables), init is not None),
        in_specs=[WHOLE] * len(args),
        out_specs=WHOLE,
        scratch_shapes=[pltpu.VMEM((nstate, width), jnp.float32)],
        out_shape=jax.ShapeDtypeStruct((nstate, width), dtype),
        cost_estimate=pl.CostEstimate(
            flops=2 * len(lefts) * nstate * g * width,
            bytes_accessed=2 * len(lefts) * g * (width + nstate),
            transcendentals=0,
        ),
        compiler_params=pltpu.CompilerParams(vmem_limit_bytes=VMEM_LIMIT),
        name="fold",
    )(*args)


def xor_pairs(n, d):
    return [(i, i ^ d) for i in range(n)]


def gather_xor(piece, axis):
    n = lax.axis_size(axis)
    if n & (n - 1):
        me = lax.axis_index(axis)
        every = lax.all_gather(piece, axis, axis=0)
        return [
            lax.dynamic_index_in_dim(every, (me + d) % n, 0, False) for d in range(n)
        ], lambda d, me: (me + d) % n
    found = [piece] + [lax.ppermute(piece, axis, xor_pairs(n, d)) for d in range(1, n)]
    return found, lambda d, me: d ^ me


def is_line(ncol):
    return ncol == 4


def body(freq_index, band_energy, pole_amp, pole_freq, left_pieces, right_pieces):
    bpiece, nstate = left_pieces.shape[:2]
    nfreq = freq_index.shape[0]
    nband, nrow, ncol = (lax.axis_size(a) for a in ("band", "row", "col"))
    axes = ("row", "col", "band")
    line = is_line(ncol)

    rights, whose = gather_xor(right_pieces, "row")
    if nrow & (nrow - 1):
        table_of = lambda q, row: (q + nrow - row) % nrow
    else:
        table_of = lambda q, row: q ^ row

    def pieces(left, owner, use=None):
        slot = lambda row, col, group: table_of(owner(col), row)
        return [(left[k], (slot, use, k)) for k in range(bpiece)]

    if line:
        inward = lax.ppermute(left_pieces, "col", [(0, 2), (3, 1)])
        outward = lax.ppermute(left_pieces, "col", [(1, 3), (2, 0)])
        near = lax.ppermute(left_pieces, "col", xor_pairs(4, 1))
        mid = lax.ppermute(left_pieces, "col", [(1, 2), (2, 1)])
        hop = lax.ppermute(inward, "col", [(2, 3), (1, 0)])
        inner = lambda row, col, group: (col == 1) | (col == 2)
        outer = lambda row, col, group: (col == 0) | (col == 3)
        soon = (
            pieces(left_pieces, lambda col: col)
            + pieces(near, lambda col: col ^ 1)
            + pieces(inward, lambda col: col ^ 2, inner)
            + pieces(outward, lambda col: col ^ 2, outer)
        )
        last = pieces(mid, lambda col: col ^ 3, inner) + pieces(hop, lambda col: col ^ 3, outer)
    else:
        lefts, owner_of = gather_xor(left_pieces, "col")
        last = [
            p
            for d, left in enumerate(lefts)
            for p in pieces(left, lambda col, d=d: owner_of(d, col))
        ]

    scalars = freq_index, band_energy
    ahead, amp, freq = screen(whose, nband, bpiece, *scalars, pole_amp, pole_freq)
    later = screen_more(whose, nband, nrow - 2, bpiece, *scalars, amp, freq)
    tables = []
    for d in range(nrow):
        source, first = (ahead, d) if d < 2 else (later, d - 2)
        held = [rights[d][k] for k in range(bpiece)]
        tables.append(apply_rights(source, first * bpiece, held))

    total = None
    if line:
        total = fold(soon, tables, None, nstate, jnp.float32)
    total = fold(last, tables, total, nstate, jnp.bfloat16)
    parts = lax.all_to_all(total, axes, split_axis=0, concat_axis=0, tiled=True)
    ndev = lax.axis_size(axes)
    owned = nstate // ndev
    mine = jnp.sum(parts.reshape(ndev, owned, nfreq, nstate).astype(jnp.float32), axis=0)
    return mine.transpose(1, 0, 2)


def solution(mesh):
    in_specs = (
        P(),
        P(),
        P("row", "col"),
        P("row", "col"),
        P(("col", "band"), None, "row"),
        P(("row", "band"), None, "col"),
    )
    out_specs = P(None, ("row", "col", "band"), None)

    return jax.shard_map(body, mesh=mesh, in_specs=in_specs, out_specs=out_specs, check_vma=False)
```
